256 devices in a mesh: expert: 16 (over y, x), wide: 16 (over z, core).
Axes of the slice: x: 4, y: 4, z: 8, core: 2. Of those that a mesh axis runs over, the one named last changes fastest.
Arguments:
- tokens: bfloat16 [32768, 2048], P(('expert', 'wide')), may hold values from -6 to 6
- out_grad: bfloat16 [32768, 2048], P(('expert', 'wide')), may hold values from -6 to 6
- routes: int32 [32768, 2], P(('expert', 'wide')), may hold values from 0 to 15, all different within a row; in each aligned block of 128 rows (0 to 127, 128 to 255, ...) at most 32 rows name the same one
- gate_prob: float32 [32768, 2], P(('expert', 'wide')), may hold values from 0.1 to 1
- w_gate: bfloat16 [16, 2048, 768], P('expert', 'wide'), may hold values from -0.125 to 0.125
- w_up: bfloat16 [16, 2048, 768], P('expert', 'wide'), may hold values from -0.125 to 0.125
- w_down: bfloat16 [16, 2048, 768], P('expert', 'wide'), may hold values from -0.21875 to 0.21875
Outputs:
- grad_input: bfloat16 [32768, 2048], P(('expert', 'wide'))
- grad_gate: float32 [16, 2048, 768], P('expert', 'wide')
- grad_up: float32 [16, 2048, 768], P('expert', 'wide')
- grad_down: float32 [16, 2048, 768], P('expert', 'wide')
The draws below stay inside these ranges and needn't reach their ends.
Inputs may be any that keep to these rules, and one draw needn't show every extreme that they name: `routes`: each row names 2 different experts; the 128 rows of one device name one expert at most 32 times, and in every draw some device names some expert exactly 32 times.
All inputs are finite; a program needn't handle non-finite values.
Results may differ from the reference program's by a relative error of at most 0.017.
Values may be sent and summed in bfloat16 or wider, within the bound.
A program may use at most 128 MiB of HBM per device.

```python
import math
import jax
import jax.numpy as jnp
import numpy as np
from jax import lax

D = 2048
F = 768
TOK_DEV = 128
TOP = 2
EXPERTS = 16
CAP = 32
TOKENS = 32768
N_EXPERT = 16
N_WIDE = 16


def shard_levels(rng, shape, shards, least, high):
    def one(dim, blocks):
        draws = jax.random.uniform(jax.random.fold_in(jax.random.fold_in(rng, 6), dim), (blocks,), jnp.float32, least / len(shards), high / len(shards))
        return jnp.repeat(jnp.exp(draws), shape[dim] // blocks).reshape((-1,) + (1,) * (len(shape) - dim - 1))

    loudness = one(*shards[0])
    for cut in shards[1:]:
        loudness = loudness * one(*cut)
    return loudness


def deal_out(own_key, own, number, rows, number_of, top, most, lean):
    order = jax.random.permutation(own_key, number_of)
    packed, ordinary = portions_of(number_of, rows * top, most, lean, True), portions_of(number_of, rows * top, most, lean, False)
    places = jnp.arange(number_of)

    def named(lengths, rotation):
        used = int((lengths > 0).sum())
        fixed = max(1, used // 4)
        shifted = fixed + (places - fixed + rotation * (used - fixed)) % max(1, number_of - fixed)
        return jnp.zeros((number_of,), jnp.int32).at[order[jnp.where(places < fixed, places, shifted)]].set(jnp.asarray(lengths, jnp.int32))

    lengths = jnp.where(number % 4 == 0, named(packed, number // 4), named(ordinary, number - number // 4 - 1))
    mixed = jax.random.permutation(jax.random.fold_in(own, 3), number_of)
    source_of, receiver = mixed[0:number_of // 2 * 2:2], mixed[1:number_of // 2 * 2:2]
    margin = jnp.minimum(lengths[source_of] - 1, most - lengths[receiver]) // 2
    margin = jnp.where((source_of == order[0]) | (receiver == order[0]) | (lengths[receiver] == 0), 0, jnp.maximum(margin, 0))
    shifted = jax.random.randint(jax.random.fold_in(own, 4), (number_of // 2,), 0, 1 << 20) % (margin + 1)
    lengths = lengths.at[source_of].add(-shifted).at[receiver].add(shifted)
    items = jnp.searchsorted(jnp.cumsum(lengths), jnp.arange(rows * top), side="right").astype(jnp.int32)
    listing = items.reshape(top, rows).T
    listing = listing[jax.random.permutation(jax.random.fold_in(own, 1), rows)]
    rotation = jax.random.randint(jax.random.fold_in(own, 2), (rows, 1), 0, top)
    return jnp.take_along_axis(listing, (jnp.arange(top)[None, :] + rotation) % top, axis=1)


def portions_of(count, total, limit, skew, full):
    portions = [(1 << 20) // math.isqrt(standing ** skew) + 1 for standing in range(1, count + 1)]
    largest = limit if full else min(limit, max(-(-total // count), total * portions[0] // sum(portions)))
    least = 1 if total - largest >= count - 1 else 0
    counts, surplus = [largest] + [least] * (count - 1), total - largest - least * (count - 1)
    while surplus > 0:
        candidates = [i for i in range(1, count) if counts[i] < largest] or [i for i in range(1, count) if counts[i] < limit]
        mass, budget = sum([portions[i] for i in candidates]), surplus
        for i in candidates:
            more = min(limit - counts[i], max(1, budget * portions[i] // mass), surplus)
            counts[i] = counts[i] + more
            surplus = surplus - more
    return np.array(counts)


def scatter_about(rng, shape, deviation, most, shards=(), kind=jnp.bfloat16):
    level = shard_levels(rng, shape, shards, -0.22, 0.18) if shards else 1.0
    drawn = jax.random.normal(rng, shape, jnp.float32) * deviation * level
    return jnp.minimum(jnp.maximum(drawn, -most), most).astype(kind)


def setup_inputs(seed: int = 0) -> dict:
    streams_of = jax.random.split(jax.random.key(seed), 8)
    tokens = scatter_about(streams_of[0], (TOKENS, D), 1.0, 6.0, ((0, 256),))
    out_grad = scatter_about(streams_of[1], (TOKENS, D), 1.0, 6.0, ((0, 256),))
    routes_keys = jax.random.split(jax.random.fold_in(streams_of[2], 1), TOKENS // TOK_DEV)
    routes_turns = jax.random.permutation(jax.random.fold_in(streams_of[2], 3), TOKENS // TOK_DEV)
    routes = jax.vmap(lambda own, number: deal_out(jax.random.fold_in(streams_of[2], 2), own, number, TOK_DEV, EXPERTS, TOP, CAP, 2))(routes_keys, routes_turns).reshape((TOKENS, TOP))
    gate_prob = jnp.clip(0.1 + 0.9 * jax.random.uniform(streams_of[3], (TOKENS, TOP), jnp.float32) ** shard_levels(streams_of[3], (TOKENS, TOP), ((0, 256),), -0.2, 0.2), 0.1, 1.0)
    w_gate = scatter_about(streams_of[4], (EXPERTS, D, F), D ** -0.5, 0.125, ((0, 16), (1, 16)))
    w_up = scatter_about(streams_of[5], (EXPERTS, D, F), D ** -0.5, 0.125, ((0, 16), (1, 16)))
    w_down = scatter_about(streams_of[6], (EXPERTS, D, F), F ** -0.5, 0.21875, ((0, 16), (1, 16)))
    return dict(tokens=tokens, out_grad=out_grad, routes=routes, gate_prob=gate_prob, w_gate=w_gate, w_up=w_up, w_down=w_down)


def swish_backward(gate_pre, up_pre, hidden_grad):
    squash = jax.nn.sigmoid(gate_pre)
    active = gate_pre * squash
    hidden = (active * up_pre).astype(jnp.bfloat16)
    gate_act = (hidden_grad * up_pre * squash * (1.0 + gate_pre * (1.0 - squash))).astype(jnp.bfloat16)
    up_act = (hidden_grad * active).astype(jnp.bfloat16)
    return hidden, gate_act, up_act


def grouped_sum(left, right):
    left_f = left.astype(jnp.float32).reshape(N_EXPERT, N_WIDE, CAP, left.shape[1])
    right_f = right.astype(jnp.float32).reshape(N_EXPERT, N_WIDE, CAP, right.shape[1])
    partial_sums = jnp.einsum("ewcd,ewcf->wdf", left_f, right_f, precision=lax.Precision.HIGHEST)
    rounded = lax.optimization_barrier(partial_sums.astype(jnp.bfloat16))
    return jnp.sum(rounded.astype(jnp.float32), axis=0)


def reference(tokens, out_grad, routes, gate_prob, w_gate, w_up, w_down):
    device_count = TOKENS // TOK_DEV
    route_count = TOK_DEV * TOP
    block_routes = routes.reshape(device_count, route_count)
    one_hot = (block_routes[:, :, None] == jnp.arange(EXPERTS, dtype=jnp.int32)[None, None, :]).astype(jnp.int32)
    before = jnp.cumsum(one_hot, axis=1) - one_hot
    slot_index = jnp.sum(before * one_hot, axis=2)
    device_ids = jnp.arange(device_count, dtype=jnp.int32)[:, None]
    row_index = (device_ids * CAP + slot_index).reshape(-1)
    token_ids = (device_ids * TOK_DEV + jnp.arange(route_count, dtype=jnp.int32)[None, :] // TOP).reshape(-1)
    expert_ids = block_routes.reshape(-1)
    gate_flat = gate_prob.reshape(-1)
    row_total = device_count * CAP

    def one_expert(carry, expert):
        target = jnp.where(expert_ids == expert, row_index, row_total).astype(jnp.int32)
        slot_token = jnp.zeros((row_total,), jnp.int32).at[target].set(token_ids, mode="drop")
        slot_gate = jnp.zeros((row_total,), jnp.float32).at[target].set(gate_flat, mode="drop")
        live_rows = jnp.zeros((row_total,), jnp.float32).at[target].set(1.0, mode="drop")
        xin = jnp.where(live_rows[:, None] > 0, tokens[slot_token], jnp.zeros((), jnp.bfloat16))
        scaled = (out_grad[slot_token].astype(jnp.float32) * slot_gate[:, None]).astype(jnp.bfloat16)
        gate_w = w_gate[expert]
        up_w = w_up[expert]
        down_w = w_down[expert]
        gate_pre = jnp.dot(xin, gate_w, preferred_element_type=jnp.float32)
        up_pre = jnp.dot(xin, up_w, preferred_element_type=jnp.float32)
        hidden_grad = jnp.dot(scaled, down_w, preferred_element_type=jnp.float32)
        hidden, gate_act, up_act = swish_backward(gate_pre, up_pre, hidden_grad)
        route_grad = (jnp.dot(gate_act, gate_w.T, preferred_element_type=jnp.float32)
                      + jnp.dot(up_act, up_w.T, preferred_element_type=jnp.float32)).astype(jnp.bfloat16)
        added = jnp.where(live_rows[:, None] > 0, route_grad.astype(jnp.float32), 0.0)
        carry = carry.at[slot_token].add(added)
        grads = (grouped_sum(xin, gate_act), grouped_sum(xin, up_act), grouped_sum(scaled, hidden))
        return carry, grads

    start = jnp.zeros((TOKENS, D), jnp.float32)
    total, grads = lax.scan(one_expert, start, jnp.arange(EXPERTS, dtype=jnp.int32))
    return total.astype(jnp.bfloat16), grads[0], grads[1], grads[2]
```

```python
import functools

import jax
import jax.numpy as jnp
from jax import lax
from jax.experimental import pallas as pl
from jax.experimental.pallas import tpu as pltpu
from jax.sharding import PartitionSpec as P

MESH = pl.DeviceIdType.MESH
BF16 = jnp.bfloat16
F32 = jnp.float32
SIDE = 4
EXPERTS = 16
RING = 8
TOK = 128
CAP = 32
ROWS = EXPERTS * CAP
D = 2048
F = 768
HALF = F // 2
BLK = 128
TRIP = 3 * HALF

OFFSETS = sorted(
    [(dy, dx) for dy in range(SIDE) for dx in range(SIDE) if (dy, dx) != (0, 0)],
    key=lambda o: -(min(o[0], SIDE - o[0]) + min(o[1], SIDE - o[1])),
)


def contract(a, b, da, db):
    return lax.dot_general(a, b, (((da,), (db,)), ((), ())), preferred_element_type=F32)


def kernel(
    tok_ref, og_ref, rt_ref, gp_ref, wg_ref, wu_ref, wd_ref,
    gi_ref, gg_ref, gu_ref, gd_ref,
    send_x, send_g, x_ref, g_ref, w_ref, w_other, pt_ref,
    pre_ref, hg_ref, act_ref, hid_ref,
    rs_send, rs_recv, fin_send, fin_recv, own_ref,
    ig_send, ig_recv, ig_own, rg_ref, ret_ref,
    xs_sem, xr_sem, gs_sem, gr_sem, xfs_sem, xfr_sem, gfs_sem, gfr_sem,
    wo_sem, ag_ssem, ag_rsem, rs_ssem, rs_rsem, fin_sem, ig_sem, ret_ssem, ret_rsem,
):
    e = lax.axis_index("expert")
    w = lax.axis_index("wide")
    ey, ex = e // SIDE, lax.rem(e, SIDE)
    z, c = w // 2, lax.rem(w, 2)
    other = 1 - c
    partner = (e, z * 2 + other)

    def zdev(step):
        return (e, lax.rem(z + step + RING, RING) * 2 + c)

    def edev(dy, dx):
        return lax.rem(ey + dy + SIDE, SIDE) * SIDE + lax.rem(ex + dx + SIDE, SIDE)

    def remote(src, dst, ssem, rsem, dev):
        return pltpu.make_async_remote_copy(
            src_ref=src, dst_ref=dst, send_sem=ssem, recv_sem=rsem,
            device_id=dev, device_id_type=MESH,
        )

    def feat(blk):
        return pl.ds(pl.multiple_of(blk * BLK, BLK), BLK)

    def erow(core, ei):
        return pl.ds(pl.multiple_of(core * ROWS + ei * CAP, CAP), CAP)

    barrier = pltpu.get_barrier_semaphore()
    peers = [(edev(dy, dx), w) for dy, dx in OFFSETS] + [zdev(1), zdev(-1), partner]
    for dev in peers:
        pl.semaphore_signal(barrier, inc=1, device_id=dev, device_id_type=MESH)

    mine = pl.ds(pl.multiple_of(c * HALF, BLK), HALF)
    theirs = pl.ds(pl.multiple_of(other * HALF, BLK), HALF)
    for i, ref in enumerate((wg_ref, wu_ref, wd_ref)):
        w_ref[feat(w), i * HALF:(i + 1) * HALF] = ref[:, mine]
        w_other[:, i * HALF:(i + 1) * HALF] = ref[:, theirs]

    routes = rt_ref[...]
    lane = lax.broadcasted_iota(jnp.int32, (TOK, BLK), 1)
    row = lax.broadcasted_iota(jnp.int32, (TOK, BLK), 0)
    hot = [routes[:, k:k + 1] == lane for k in range(2)]
    named = jnp.where(jnp.logical_or(hot[0], hot[1]), 1.0, 0.0).astype(BF16)
    earlier = jnp.where(lane < row, 1.0, 0.0).astype(BF16)
    before = contract(earlier, named, 1, 0)
    slot_lane = lax.broadcasted_iota(jnp.int32, (TOK, ROWS), 1).astype(F32)
    picks = []
    for k in range(2):
        slot = jnp.sum(jnp.where(hot[k], before, 0.0), axis=1, keepdims=True)
        pos = routes[:, k:k + 1].astype(F32) * float(CAP) + slot
        picks.append(jnp.where(pos == slot_lane, 1.0, 0.0))
    pt_ref[...] = (picks[0] + picks[1]).astype(BF16)
    pick = jnp.transpose(picks[0] + picks[1]).astype(BF16)
    for j in range(4):
        cols = slice(j * 512, (j + 1) * 512)
        send_x[:, cols] = contract(pick, tok_ref[:, cols], 1, 0).astype(BF16)

    pl.semaphore_wait(barrier, len(peers))

    swap = remote(w_other, w_ref.at[feat(w)], wo_sem.at[0], wo_sem.at[1], partner)
    swap.start()

    def ag_block(direction, k):
        parity = c if (k % 2 == 0) else other
        if k == 6 and direction < 0:
            parity = other
        blk = lax.rem(z - direction * (k // 2) + 2 * RING, RING)
        return blk * 2 + parity

    def ag_copy(direction, k):
        d = 0 if direction > 0 else 1
        blk = ag_block(direction, k)
        return remote(
            w_ref.at[feat(blk)], w_ref.at[feat(blk)],
            ag_ssem.at[d, k], ag_rsem.at[d, k], zdev(direction),
        )

    ag_copy(1, 0).start()
    ag_copy(-1, 0).start()

    def row_copies(src, dst, ssem, rsem):
        out = []
        for i, (dy, dx) in enumerate(OFFSETS):
            dest = edev(dy, dx)
            out.append(remote(
                src.at[pl.ds(pl.multiple_of(dest * CAP, CAP), CAP)],
                dst.at[erow(c, e)], ssem.at[i], rsem.at[i], (dest, w),
            ))
        return out

    x_sends = row_copies(send_x, x_ref, xs_sem, xr_sem)
    for copy in x_sends:
        copy.start()
    swap.wait()
    ag_copy(1, 1).start()
    ag_copy(-1, 1).start()

    pick_two = jnp.concatenate([jnp.transpose(p).astype(BF16) for p in picks], axis=1)
    gates = [gp_ref[:, k:k + 1] for k in range(2)]
    for j in range(4):
        cols = slice(j * 512, (j + 1) * 512)
        part = og_ref[:, cols].astype(F32)
        both = jnp.concatenate([(part * gates[k]).astype(BF16) for k in range(2)], axis=0)
        send_g[:, cols] = contract(pick_two, both, 1, 0).astype(BF16)
    g_sends = row_copies(send_g, g_ref, gs_sem, gr_sem)
    for copy in g_sends:
        copy.start()

    own_rows = pl.ds(pl.multiple_of(e * CAP, CAP), CAP)
    x_ref[erow(c, e), :] = send_x[own_rows, :]
    g_ref[erow(c, e), :] = send_g[own_rows, :]

    def forward(buf, ssem, rsem, i, src):
        return remote(buf.at[erow(c, src)], buf.at[erow(c, src)], ssem.at[i], rsem.at[i], partner)

    for k in range(7):
        for direction in (1, -1):
            ag_copy(direction, k).wait_recv()
            nxt = k + 2
            if direction < 0 and k == 5:
                ag_copy(direction, 6).start()
            elif nxt <= 6 and not (direction < 0 and k == 4):
                ag_copy(direction, nxt).start()
        if k == 1:
            forward(x_ref, xfs_sem, xfr_sem, 15, e).start()
            forward(g_ref, gfs_sem, gfr_sem, 15, e).start()

    def pass_on(buf, sends, ssem, rsem):
        for i, (dy, dx) in enumerate(OFFSETS):
            sends[i].wait_recv()
            forward(buf, ssem, rsem, i, edev(-dy, -dx)).start()

    def arrived(buf, ssem, rsem):
        for i, (dy, dx) in enumerate(OFFSETS + [(0, 0)]):
            forward(buf, ssem, rsem, i, edev(-dy, -dx)).wait_recv()

    pass_on(x_ref, x_sends, xfs_sem, xfr_sem)
    arrived(x_ref, xfs_sem, xfr_sem)

    def first(t, carry):
        rows = pl.ds(pl.multiple_of((t // 3) * 512, 512), 512)
        cols = pl.ds(pl.multiple_of(lax.rem(t, 3) * 256, 256), 256)
        pre_ref[rows, cols] = contract(x_ref[rows, :], w_ref[:, cols], 1, 0)
        return carry

    lax.fori_loop(0, 6, first, 0)

    pass_on(g_ref, g_sends, gfs_sem, gfr_sem)
    arrived(g_ref, gfs_sem, gfr_sem)

    def second(t, carry):
        rows = pl.ds(pl.multiple_of(t * 512, 512), 512)
        hg_ref[rows, :] = contract(g_ref[rows, :], w_ref[:, 2 * HALF:], 1, 0)
        return carry

    lax.fori_loop(0, 2, second, 0)

    def swish(t, carry):
        rows = pl.ds(pl.multiple_of(t * 32, 32), 32)
        gate_pre = pre_ref[rows, :HALF]
        up_pre = pre_ref[rows, HALF:]
        hidden_grad = hg_ref[rows, :]
        squash = jax.nn.sigmoid(gate_pre)
        active = gate_pre * squash
        hid_ref[rows, :] = (active * up_pre).astype(BF16)
        act_ref[rows, :HALF] = (
            hidden_grad * up_pre * squash * (1.0 + gate_pre * (1.0 - squash))
        ).astype(BF16)
        act_ref[rows, HALF:] = (hidden_grad * active).astype(BF16)
        return carry

    lax.fori_loop(0, 2 * ROWS // 32, swish, 0)

    def rs_chunk(direction, k):
        dist = 4 - (k + 1) // 2
        even = lax.rem(k, 2) == 0
        if direction > 0:
            parity = jnp.where(even, c, other)
        else:
            parity = jnp.where(even, other, c)
        return lax.rem(z + direction * dist + RING, RING) * 2 + parity

    def partial(blk):
        cols = feat(blk)
        left = contract(x_ref[:, cols], act_ref[...], 0, 0)
        right = contract(g_ref[:, cols], hid_ref[...], 0, 0)
        return left, right

    def rs_copy(direction, k):
        d = 0 if direction > 0 else 1
        return remote(
            rs_send.at[d, k], rs_recv.at[d, k], rs_ssem.at[d, k], rs_rsem.at[d, k],
            zdev(direction),
        )

    def rs_step(k, add):
        for direction in (1, -1):
            d = 0 if direction > 0 else 1
            left, right = partial(rs_chunk(direction, k))
            if add:
                rs_copy(direction, k - 2).wait_recv()
                left = left + rs_recv[d, k - 2, :, :2 * HALF].astype(F32)
                right = right + rs_recv[d, k - 2, :, 2 * HALF:].astype(F32)
            rs_send[d, k, :, :2 * HALF] = left.astype(BF16)
            rs_send[d, k, :, 2 * HALF:] = right.astype(BF16)
            rs_copy(direction, k).start()

    def rs_first(k, carry):
        rs_step(k, False)
        return carry

    lax.fori_loop(0, 2, rs_first, 0)

    def input_part(core, j):
        rows = pl.ds(pl.multiple_of(core * ROWS, ROWS), ROWS)
        cols = pl.ds(pl.multiple_of(j * 256, 256), 256)
        return contract(act_ref[rows, :], w_ref[cols, :2 * HALF], 1, 1), cols

    def for_other(j, carry):
        got, cols = input_part(other, j)
        ig_send[:, cols] = got.astype(BF16)
        return carry

    lax.fori_loop(0, 8, for_other, 0)
    ig_copy = remote(ig_send, ig_recv, ig_sem.at[0], ig_sem.at[1], partner)
    ig_copy.start()

    def for_mine(j, carry):
        got, cols = input_part(c, j)
        ig_own[:, cols] = got
        return carry

    lax.fori_loop(0, 8, for_mine, 0)
    ig_copy.wait_recv()

    def join(t, carry):
        rows = pl.ds(pl.multiple_of(t * CAP, CAP), CAP)
        rg_ref[rows, :] = (ig_own[rows, :] + ig_recv[rows, :].astype(F32)).astype(BF16)
        return carry

    lax.fori_loop(0, EXPERTS, join, 0)
    returns = []
    for i, (dy, dx) in enumerate(OFFSETS):
        dest = edev(dy, dx)
        returns.append(remote(
            rg_ref.at[pl.ds(pl.multiple_of(dest * CAP, CAP), CAP)],
            ret_ref.at[own_rows], ret_ssem.at[i], ret_rsem.at[i], (dest, w),
        ))
    for copy in returns:
        copy.start()
    ret_ref[own_rows, :] = rg_ref[own_rows, :]

    def rs_next(k, carry):
        rs_step(k, True)
        return carry

    lax.fori_loop(2, 7, rs_next, 0)

    def keep(p, blk):
        left, right = partial(blk)
        own_ref[p, :, :2 * HALF] = left
        own_ref[p, :, 2 * HALF:] = right

    keep(0, z * 2 + c)
    keep(1, z * 2 + other)

    for copy in returns:
        copy.wait_recv()
    for j in range(4):
        cols = slice(j * 512, (j + 1) * 512)
        gi_ref[:, cols] = contract(pt_ref[...], ret_ref[:, cols], 1, 0).astype(BF16)

    rs_copy(1, 5).wait_recv()
    rs_copy(-1, 5).wait_recv()
    rs_copy(-1, 6).wait_recv()
    fin_send[...] = (
        own_ref[1] + rs_recv[0, 5].astype(F32) + rs_recv[1, 6].astype(F32)
    ).astype(BF16)
    fin = remote(fin_send, fin_recv, fin_sem.at[0], fin_sem.at[1], partner)
    fin.start()
    rs_copy(1, 6).wait_recv()
    mine_sum = own_ref[0] + rs_recv[0, 6].astype(F32) + rs_recv[1, 5].astype(F32)
    for i, ref in enumerate((gg_ref, gu_ref, gd_ref)):
        ref[:, mine] = mine_sum[:, i * HALF:(i + 1) * HALF]
    fin.wait_recv()
    for i, ref in enumerate((gg_ref, gu_ref, gd_ref)):
        ref[:, theirs] = fin_recv[:, i * HALF:(i + 1) * HALF].astype(F32)

    for copy in x_sends + g_sends + returns:
        copy.wait_send()
    for i, (dy, dx) in enumerate(OFFSETS + [(0, 0)]):
        src = edev(-dy, -dx)
        forward(x_ref, xfs_sem, xfr_sem, i, src).wait_send()
        forward(g_ref, gfs_sem, gfr_sem, i, src).wait_send()
    for direction in (1, -1):
        for k in range(7):
            ag_copy(direction, k).wait_send()
            rs_copy(direction, k).wait_send()
    ig_copy.wait_send()
    fin.wait_send()


def on_device(tokens, out_grad, routes, gate_prob, w_gate, w_up, w_down):
    flat = [a.reshape(BLK, F) for a in (w_gate, w_up, w_down)]
    dma = pltpu.SemaphoreType.DMA
    vmem = pl.BlockSpec(memory_space=pltpu.VMEM)
    outs = pl.pallas_call(
        kernel,
        name="moe_back",
        out_shape=(
            jax.ShapeDtypeStruct((TOK, D), BF16),
            jax.ShapeDtypeStruct((BLK, F), F32),
            jax.ShapeDtypeStruct((BLK, F), F32),
            jax.ShapeDtypeStruct((BLK, F), F32),
        ),
        in_specs=[vmem] * 7,
        out_specs=(vmem,) * 4,
        scratch_shapes=[
            pltpu.VMEM((ROWS, D), BF16),
            pltpu.VMEM((ROWS, D), BF16),
            pltpu.VMEM((2 * ROWS, D), BF16),
            pltpu.VMEM((2 * ROWS, D), BF16),
            pltpu.VMEM((D, TRIP), BF16),
            pltpu.VMEM((BLK, TRIP), BF16),
            pltpu.VMEM((TOK, ROWS), BF16),
            pltpu.VMEM((2 * ROWS, F), F32),
            pltpu.VMEM((2 * ROWS, HALF), F32),
            pltpu.VMEM((2 * ROWS, F), BF16),
            pltpu.VMEM((2 * ROWS, HALF), BF16),
            pltpu.VMEM((2, 7, BLK, TRIP), BF16),
            pltpu.VMEM((2, 7, BLK, TRIP), BF16),
            pltpu.VMEM((BLK, TRIP), BF16),
            pltpu.VMEM((BLK, TRIP), BF16),
            pltpu.VMEM((2, BLK, TRIP), F32),
            pltpu.VMEM((ROWS, D), BF16),
            pltpu.VMEM((ROWS, D), BF16),
            pltpu.VMEM((ROWS, D), F32),
            pltpu.VMEM((ROWS, D), BF16),
            pltpu.VMEM((ROWS, D), BF16),
            dma((15,)), dma((15,)), dma((15,)), dma((15,)),
            dma((16,)), dma((16,)), dma((16,)), dma((16,)),
            dma((2,)), dma((2, 7)), dma((2, 7)), dma((2, 7)), dma((2, 7)),
            dma((2,)), dma((2,)), dma((15,)), dma((15,)),
        ],
        compiler_params=pltpu.CompilerParams(
            collective_id=0, has_side_effects=True, vmem_limit_bytes=67043328,
        ),
    )(tokens, out_grad, routes, gate_prob, *flat)
    return (outs[0],) + tuple(o[None] for o in outs[1:])


def solution(mesh):
    rows = P(("expert", "wide"), None)
    weight = P("expert", "wide", None)
    return jax.shard_map(
        on_device,
        mesh=mesh,
        in_specs=(rows,) * 4 + (weight,) * 3,
        out_specs=(rows,) + (weight,) * 3,
        check_vma=False,
    )
```

```python
import functools

import jax
import jax.numpy as jnp
from jax import lax
from jax.experimental import pallas as pl
from jax.experimental.pallas import tpu as pltpu
from jax.sharding import PartitionSpec as P

MESH = pl.DeviceIdType.MESH
BF16 = jnp.bfloat16
F32 = jnp.float32
SIDE = 4
EXPERTS = 16
RING = 8
TOK = 128
CAP = 32
ROWS = EXPERTS * CAP
D = 2048
F = 768
HALF = F // 2
BLK = 128
TRIP = 3 * HALF

OFFSETS = sorted(
    [(dy, dx) for dy in range(SIDE) for dx in range(SIDE) if (dy, dx) != (0, 0)],
    key=lambda o: -(min(o[0], SIDE - o[0]) + min(o[1], SIDE - o[1])),
)


def contract(a, b, da, db):
    return lax.dot_general(a, b, (((da,), (db,)), ((), ())), preferred_element_type=F32)


def kernel(
    tok_hbm, og_hbm, rt_hbm, gp_hbm, wg_hbm, wu_hbm, wd_hbm,
    gi_ref, gg_ref, gu_ref, gd_ref,
    tok_ref, og_ref, rt_ref, gp_ref,
    send_x, send_g, x_ref, g_ref, wgu_ref, wd_ref, wgu_other, wd_other, pick_ref,
    pre_ref, hg_ref, act_ref, hid_ref,
    sd_send, sd_recv, su_send, su_recv, fin_send, fin_recv, own_ref,
    ig_send, ig_recv, ig_own, rg_ref, ret_ref,
    in_sem, xs_sem, xr_sem, gs_sem, gr_sem, xfs_sem, xfr_sem, gfs_sem, gfr_sem,
    wo_ssem, wo_rsem, ag_ssem, ag_rsem, rs_ssem, rs_rsem, fin_sem, ig_sem, ret_ssem, ret_rsem,
):
    e = lax.axis_index("expert")
    w = lax.axis_index("wide")
    ey, ex = e // SIDE, lax.rem(e, SIDE)
    z, c = w // 2, lax.rem(w, 2)
    other = 1 - c
    partner = (e, z * 2 + other)

    def zdev(step, core):
        return (e, lax.rem(z + step + RING, RING) * 2 + core)

    def edev(dy, dx):
        return lax.rem(ey + dy + SIDE, SIDE) * SIDE + lax.rem(ex + dx + SIDE, SIDE)

    def remote(src, dst, ssem, rsem, dev):
        return pltpu.make_async_remote_copy(
            src_ref=src, dst_ref=dst, send_sem=ssem, recv_sem=rsem,
            device_id=dev, device_id_type=MESH,
        )

    def feat(blk):
        return pl.ds(pl.multiple_of(blk * BLK, BLK), BLK)

    def erow(core, ei):
        return pl.ds(pl.multiple_of(core * ROWS + ei * CAP, CAP), CAP)

    barrier = pltpu.get_barrier_semaphore()
    peers = [(edev(dy, dx), w) for dy, dx in OFFSETS] + [partner]
    peers += [zdev(s, core) for s in (1, -1) for core in (c, other)]
    for dev in peers:
        pl.semaphore_signal(barrier, inc=1, device_id=dev, device_id_type=MESH)

    mine = pl.ds(pl.multiple_of(c * HALF, BLK), HALF)
    theirs = pl.ds(pl.multiple_of(other * HALF, BLK), HALF)
    places = [
        (rt_hbm, rt_ref), (gp_hbm, gp_ref), (tok_hbm, tok_ref),
        (wg_hbm.at[:, mine], wgu_ref.at[feat(w), pl.ds(0, HALF)]),
        (wu_hbm.at[:, mine], wgu_ref.at[feat(w), pl.ds(HALF, HALF)]),
        (wg_hbm.at[:, theirs], wgu_other.at[:, pl.ds(0, HALF)]),
        (wu_hbm.at[:, theirs], wgu_other.at[:, pl.ds(HALF, HALF)]),
        (wd_hbm.at[:, mine], wd_ref.at[feat(w)]),
        (wd_hbm.at[:, theirs], wd_other),
        (og_hbm, og_ref),
    ]
    loads = [pltpu.make_async_copy(a, b, in_sem.at[i]) for i, (a, b) in enumerate(places)]
    for load in loads:
        load.start()

    loads[0].wait()
    loads[1].wait()
    lane = lax.broadcasted_iota(jnp.int32, (EXPERTS, TOK), 0)
    hot = [rt_ref[k:k + 1, :] == lane for k in range(2)]
    named = jnp.where(jnp.logical_or(hot[0], hot[1]), 1.0, 0.0).astype(BF16)
    earlier = jnp.where(
        lax.broadcasted_iota(jnp.int32, (TOK, TOK), 0)
        < lax.broadcasted_iota(jnp.int32, (TOK, TOK), 1), 1.0, 0.0,
    ).astype(BF16)
    before = contract(named, earlier, 1, 0)
    slots = lax.broadcasted_iota(jnp.int32, (ROWS, TOK), 0).astype(F32)
    pick, slot_gate = 0.0, 0.0
    for k in range(2):
        slot = jnp.sum(jnp.where(hot[k], before, 0.0), axis=0, keepdims=True)
        pos = rt_ref[k:k + 1, :].astype(F32) * float(CAP) + slot
        chosen = pos == slots
        pick = pick + jnp.where(chosen, 1.0, 0.0)
        slot_gate = slot_gate + jnp.where(chosen, gp_ref[k:k + 1, :], 0.0)
    slot_gate = jnp.sum(slot_gate, axis=1, keepdims=True)
    pick_ref[...] = pick.astype(BF16)
    loads[2].wait()

    def pick_x(j, carry):
        cols = pl.ds(pl.multiple_of(j * 512, 512), 512)
        send_x[:, cols] = contract(pick_ref[...], tok_ref[:, cols], 1, 0).astype(BF16)
        return carry

    lax.fori_loop(0, 4, pick_x, 0)
    for load in loads[3:9]:
        load.wait()
    pl.semaphore_wait(barrier, len(peers))

    swaps = [
        remote(wgu_other, wgu_ref.at[feat(w)], wo_ssem.at[0], wo_rsem.at[0], partner),
        remote(wd_other, wd_ref.at[feat(w)], wo_ssem.at[1], wo_rsem.at[1], partner),
    ]
    for swap in swaps:
        swap.start()

    def ag_copy(kind, direction, k):
        d = 0 if direction > 0 else 1
        parity = c if (k % 2 == 0) else other
        if k == 6 and direction < 0:
            parity = other
        blk = lax.rem(z - direction * (k // 2) + 2 * RING, RING) * 2 + parity
        ref = (wgu_ref, wd_ref)[kind].at[feat(blk)]
        i = kind * 7 + k
        return remote(ref, ref, ag_ssem.at[d, i], ag_rsem.at[d, i], zdev(direction, c))

    for kind in range(2):
        for direction in (1, -1):
            ag_copy(kind, direction, 0).start()

    own_rows = pl.ds(pl.multiple_of(e * CAP, CAP), CAP)

    def row_copies(src, dst, ssem, rsem):
        out = []
        for i, (dy, dx) in enumerate(OFFSETS):
            dest = edev(dy, dx)
            out.append(remote(
                src.at[pl.ds(pl.multiple_of(dest * CAP, CAP), CAP)],
                dst.at[erow(c, e)], ssem.at[i], rsem.at[i], (dest, w),
            ))
        return out

    x_sends = row_copies(send_x, x_ref, xs_sem, xr_sem)
    for copy in x_sends:
        copy.start()
    x_ref[erow(c, e), :] = send_x[own_rows, :]

    loads[9].wait()

    def pick_g(j, carry):
        cols = pl.ds(pl.multiple_of(j * 512, 512), 512)
        got = contract(pick_ref[...], og_ref[:, cols], 1, 0)
        send_g[:, cols] = (got * slot_gate).astype(BF16)
        return carry

    lax.fori_loop(0, 4, pick_g, 0)
    g_sends = row_copies(send_g, g_ref, gs_sem, gr_sem)
    for copy in g_sends:
        copy.start()
    g_ref[erow(c, e), :] = send_g[own_rows, :]
    for kind in range(2):
        swaps[kind].wait()
        for direction in (1, -1):
            ag_copy(kind, direction, 1).start()

    def forward(buf, ssem, rsem, i, src):
        return remote(buf.at[erow(c, src)], buf.at[erow(c, src)], ssem.at[i], rsem.at[i], partner)

    def pass_on(buf, sends, ssem, rsem, lo, hi):
        for i in range(lo, hi):
            dy, dx = OFFSETS[i]
            sends[i].wait_recv()
            forward(buf, ssem, rsem, i, edev(-dy, -dx)).start()

    def pass_x(lo, hi):
        pass_on(x_ref, x_sends, xfs_sem, xfr_sem, lo, hi)

    def pass_g(lo, hi):
        pass_on(g_ref, g_sends, gfs_sem, gfr_sem, lo, hi)

    def arrived(buf, ssem, rsem):
        for i, (dy, dx) in enumerate(OFFSETS + [(0, 0)]):
            forward(buf, ssem, rsem, i, edev(-dy, -dx)).wait_recv()

    def ag_arrive(kind, k):
        for direction in (1, -1):
            ag_copy(kind, direction, k).wait_recv()
            if direction < 0 and k == 5:
                ag_copy(kind, direction, 6).start()
            elif k + 2 <= 6 and not (direction < 0 and k == 4):
                ag_copy(kind, direction, k + 2).start()

    def add_block(blk, start):
        feats = pl.ds(pl.multiple_of(lax.rem(blk, RING) * 256, 256), 256)

        def tile(t, carry):
            rows = pl.ds(pl.multiple_of(t * 256, 256), 256)
            got = contract(x_ref[rows, feats], wgu_ref[feats, :], 1, 0)
            pre_ref[rows, :] = got if start else pre_ref[rows, :] + got
            return carry

        lax.fori_loop(0, 4, tile, 0)

    def add_more(t, carry):
        add_block(z + RING - 3 + t, False)
        return carry

    def hidden(t, carry):
        rows = pl.ds(pl.multiple_of(t * 32, 32), 32)
        gate_pre = pre_ref[rows, :HALF]
        active = gate_pre * jax.nn.sigmoid(gate_pre)
        hid_ref[rows, :] = (active * pre_ref[rows, HALF:]).astype(BF16)
        return carry

    for k in range(5):
        ag_arrive(0, k)
        ag_arrive(1, k)
        if k == 0:
            forward(x_ref, xfs_sem, xfr_sem, 15, e).start()
            forward(g_ref, gfs_sem, gfr_sem, 15, e).start()
        if k == 3:
            pass_x(0, 8)
        if k == 4:
            pass_x(8, 15)
    ag_arrive(0, 5)
    arrived(x_ref, xfs_sem, xfr_sem)
    add_block(z, True)
    lax.fori_loop(0, 3, add_more, 0)
    ag_arrive(1, 5)
    lax.fori_loop(4, 7, add_more, 0)
    pass_g(0, 6)
    ag_arrive(0, 6)
    add_block(z + 4, False)
    lax.fori_loop(0, 2 * ROWS // 32, hidden, 0)
    ag_arrive(1, 6)
    pass_g(6, 15)
    arrived(g_ref, gfs_sem, gfr_sem)

    bufs = ((sd_send, sd_recv), (su_send, su_recv))

    def partial(kind, blk):
        cols = feat(blk)
        if kind == 0:
            return contract(g_ref[:, cols], hid_ref[...], 0, 0)
        return contract(x_ref[:, cols], act_ref[...], 0, 0)

    def rs_parity(direction, k):
        even = lax.rem(k, 2) == 0
        return jnp.where(even, c, other) if direction > 0 else jnp.where(even, other, c)

    def rs_copy(kind, direction, k):
        d = 0 if direction > 0 else 1
        send, recv = bufs[kind]
        core = jnp.where(k >= 5, rs_parity(direction, k), c)
        return remote(
            send.at[d, k], recv.at[d, k], rs_ssem.at[d, kind * 7 + k],
            rs_rsem.at[d, kind * 7 + k], zdev(direction, core),
        )

    def rs_step(kind, k, add):
        send, recv = bufs[kind]
        for direction in (1, -1):
            d = 0 if direction > 0 else 1
            dist = 4 - (k + 1) // 2
            blk = lax.rem(z + direction * dist + RING, RING) * 2 + rs_parity(direction, k)
            got = partial(kind, blk)
            if add:
                rs_copy(kind, direction, k - 2).wait_recv()
                got = got + recv[d, k - 2].astype(F32)
            send[d, k] = got.astype(BF16)
            rs_copy(kind, direction, k).start()

    def rs_loop(kind, lo, hi, add):
        def step(k, carry):
            rs_step(kind, k, add)
            return carry

        lax.fori_loop(lo, hi, step, 0)

    rs_loop(0, 0, 2, False)

    def second(t, carry):
        rows = pl.ds(pl.multiple_of(t * 512, 512), 512)
        hg_ref[rows, :] = contract(g_ref[rows, :], wd_ref[...], 1, 0)
        return carry

    lax.fori_loop(0, 2, second, 0)

    def swish(t, carry):
        rows = pl.ds(pl.multiple_of(t * 32, 32), 32)
        gate_pre = pre_ref[rows, :HALF]
        up_pre = pre_ref[rows, HALF:]
        hidden_grad = hg_ref[rows, :]
        squash = jax.nn.sigmoid(gate_pre)
        act_ref[rows, :HALF] = (
            hidden_grad * up_pre * squash * (1.0 + gate_pre * (1.0 - squash))
        ).astype(BF16)
        act_ref[rows, HALF:] = (hidden_grad * (gate_pre * squash)).astype(BF16)
        return carry

    lax.fori_loop(0, 2 * ROWS // 32, swish, 0)
    rs_loop(1, 0, 2, False)

    def input_part(core, j):
        rows = pl.ds(pl.multiple_of(core * ROWS, ROWS), ROWS)
        cols = pl.ds(pl.multiple_of(j * 256, 256), 256)
        return contract(act_ref[rows, :], wgu_ref[cols, :], 1, 1), cols

    def for_other(j, carry):
        got, cols = input_part(other, j)
        ig_send[:, cols] = got.astype(BF16)
        return carry

    lax.fori_loop(0, 8, for_other, 0)
    ig_copy = remote(ig_send, ig_recv, ig_sem.at[0], ig_sem.at[1], partner)
    ig_copy.start()
    rs_loop(0, 2, 4, True)

    def for_mine(j, carry):
        got, cols = input_part(c, j)
        ig_own[:, cols] = got
        return carry

    lax.fori_loop(0, 8, for_mine, 0)
    ig_copy.wait_recv()

    def join(t, carry):
        rows = pl.ds(pl.multiple_of(t * CAP, CAP), CAP)
        rg_ref[rows, :] = (ig_own[rows, :] + ig_recv[rows, :].astype(F32)).astype(BF16)
        return carry

    lax.fori_loop(0, EXPERTS, join, 0)
    returns = []
    for i, (dy, dx) in enumerate(OFFSETS):
        dest = edev(dy, dx)
        returns.append(remote(
            rg_ref.at[pl.ds(pl.multiple_of(dest * CAP, CAP), CAP)],
            ret_ref.at[own_rows], ret_ssem.at[i], ret_rsem.at[i], (dest, w),
        ))
    for copy in returns:
        copy.start()
    ret_ref[own_rows, :] = rg_ref[own_rows, :]

    def rs_rest(k, carry):
        rs_step(1, k, True)

        @pl.when(k <= 4)
        def _():
            rs_step(0, k + 2, True)

        return carry

    lax.fori_loop(2, 4, rs_rest, 0)

    fin_send[:, :F] = partial(1, z * 2 + other).astype(BF16)
    fin_send[:, F:] = partial(0, z * 2 + other).astype(BF16)
    fin = remote(fin_send, fin_recv, fin_sem.at[0], fin_sem.at[1], partner)
    fin.start()
    lax.fori_loop(4, 7, rs_rest, 0)
    own_ref[:, :F] = partial(1, w)
    own_ref[:, F:] = partial(0, w)

    for copy in returns:
        copy.wait_recv()

    def combine(j, carry):
        cols = pl.ds(pl.multiple_of(j * 512, 512), 512)
        gi_ref[:, cols] = contract(pick_ref[...], ret_ref[:, cols], 0, 0).astype(BF16)
        return carry

    lax.fori_loop(0, 4, combine, 0)
    fin.wait_recv()

    for kind in range(2):
        recv = bufs[kind][1]
        for direction in (1, -1):
            for k in (5, 6):
                rs_copy(kind, direction, k).wait_recv()
        outs = ((gd_ref, F),) if kind == 0 else ((gg_ref, 0), (gu_ref, HALF))
        for i, (out, lo) in enumerate(outs):
            part = slice(i * HALF, (i + 1) * HALF)
            out[:, mine] = (
                own_ref[:, lo:lo + HALF]
                + recv[0, 6, :, part].astype(F32) + recv[1, 5, :, part].astype(F32)
            )
            out[:, theirs] = (
                fin_recv[:, lo:lo + HALF].astype(F32)
                + recv[0, 5, :, part].astype(F32) + recv[1, 6, :, part].astype(F32)
            )

    for copy in x_sends + g_sends + returns:
        copy.wait_send()
    for i, (dy, dx) in enumerate(OFFSETS + [(0, 0)]):
        src = edev(-dy, -dx)
        forward(x_ref, xfs_sem, xfr_sem, i, src).wait_send()
        forward(g_ref, gfs_sem, gfr_sem, i, src).wait_send()
    for direction in (1, -1):
        for k in range(7):
            for kind in range(2):
                ag_copy(kind, direction, k).wait_send()
                rs_copy(kind, direction, k).wait_send()
    ig_copy.wait_send()
    fin.wait_send()


def store(*refs):
    n = len(refs) // 2
    sem = refs[-1]
    copies = [pltpu.make_async_copy(refs[i], refs[n + i], sem.at[i]) for i in range(n)]
    for copy in copies:
        copy.start()
    for copy in copies:
        copy.wait()


def on_device(tokens, out_grad, routes, gate_prob, w_gate, w_up, w_down):
    flat = [a.reshape(BLK, F) for a in (w_gate, w_up, w_down)]
    dma = pltpu.SemaphoreType.DMA
    vmem = pl.BlockSpec(memory_space=pltpu.VMEM)
    anyw = pl.BlockSpec(memory_space=pl.ANY)
    shapes = [((TOK, D), BF16)] + [((BLK, F), F32)] * 3
    outs = pl.pallas_call(
        kernel,
        name="moe_back",
        out_shape=tuple(pltpu.VMEM(s, t) for s, t in shapes),
        in_specs=[anyw] * 7,
        out_specs=(vmem,) * 4,
        scratch_shapes=[
            pltpu.VMEM((TOK, D), BF16),
            pltpu.VMEM((TOK, D), BF16),
            pltpu.VMEM((2, TOK), jnp.int32),
            pltpu.VMEM((2, TOK), F32),
            pltpu.VMEM((ROWS, D), BF16),
            pltpu.VMEM((ROWS, D), BF16),
            pltpu.VMEM((2 * ROWS, D), BF16),
            pltpu.VMEM((2 * ROWS, D), BF16),
            pltpu.VMEM((D, F), BF16),
            pltpu.VMEM((D, HALF), BF16),
            pltpu.VMEM((BLK, F), BF16),
            pltpu.VMEM((BLK, HALF), BF16),
            pltpu.VMEM((ROWS, TOK), BF16),
            pltpu.VMEM((2 * ROWS, F), F32),
            pltpu.VMEM((2 * ROWS, HALF), F32),
            pltpu.VMEM((2 * ROWS, F), BF16),
            pltpu.VMEM((2 * ROWS, HALF), BF16),
            pltpu.VMEM((2, 7, BLK, HALF), BF16),
            pltpu.VMEM((2, 7, BLK, HALF), BF16),
            pltpu.VMEM((2, 7, BLK, F), BF16),
            pltpu.VMEM((2, 7, BLK, F), BF16),
            pltpu.VMEM((BLK, TRIP), BF16),
            pltpu.VMEM((BLK, TRIP), BF16),
            pltpu.VMEM((BLK, TRIP), F32),
            pltpu.VMEM((ROWS, D), BF16),
            pltpu.VMEM((ROWS, D), BF16),
            pltpu.VMEM((ROWS, D), F32),
            pltpu.VMEM((ROWS, D), BF16),
            pltpu.VMEM((ROWS, D), BF16),
            dma((10,)),
            dma((15,)), dma((15,)), dma((15,)), dma((15,)),
            dma((16,)), dma((16,)), dma((16,)), dma((16,)),
            dma((2,)), dma((2,)), dma((2, 14)), dma((2, 14)), dma((2, 14)), dma((2, 14)),
            dma((2,)), dma((2,)), dma((15,)), dma((15,)),
        ],
        compiler_params=pltpu.CompilerParams(
            collective_id=0, has_side_effects=True, vmem_limit_bytes=56 << 20,
        ),
    )(tokens, out_grad, routes.T, gate_prob.T, *flat)
    outs = pl.pallas_call(
        store,
        name="store",
        out_shape=tuple(jax.ShapeDtypeStruct(s, t) for s, t in shapes),
        in_specs=[vmem] * 4,
        out_specs=(anyw,) * 4,
        scratch_shapes=[dma((4,))],
        compiler_params=pltpu.CompilerParams(vmem_limit_bytes=4 << 20),
    )(*outs)
    return (outs[0],) + tuple(o[None] for o in outs[1:])


def solution(mesh):
    rows = P(("expert", "wide"), None)
    weight = P("expert", "wide", None)
    return jax.shard_map(
        on_device,
        mesh=mesh,
        in_specs=(rows,) * 4 + (weight,) * 3,
        out_specs=(rows,) + (weight,) * 3,
        check_vma=False,
    )
```

```python
import functools

import jax
import jax.numpy as jnp
from jax import lax
from jax.experimental import pallas as pl
from jax.experimental.pallas import tpu as pltpu
from jax.sharding import PartitionSpec as P

MESH = pl.DeviceIdType.MESH
BF16 = jnp.bfloat16
F32 = jnp.float32
SIDE = 4
EXPERTS = 16
RING = 8
TOK = 128
CAP = 32
ROWS = EXPERTS * CAP
D = 2048
F = 768
HALF = F // 2
BLK = 128
TRIP = 3 * HALF

OFFSETS = sorted(
    [(dy, dx) for dy in range(SIDE) for dx in range(SIDE) if (dy, dx) != (0, 0)],
    key=lambda o: -(min(o[0], SIDE - o[0]) + min(o[1], SIDE - o[1])),
)


def contract(a, b, da, db):
    return lax.dot_general(a, b, (((da,), (db,)), ((), ())), preferred_element_type=F32)


def kernel(
    tok_hbm, og_hbm, rt_hbm, gp_hbm, wg_hbm, wu_hbm, wd_hbm,
    gi_ref, gg_ref, gu_ref, gd_ref,
    tok_ref, og_ref, rt_ref, gp_ref,
    send_x, send_g, x_ref, g_ref, wgu_ref, wd_ref, wgu_other, wd_other, pick_ref,
    pre_ref, hg_ref, act_ref, hid_ref,
    sd_send, sd_recv, su_send, su_recv, fin_send, fin_recv, own_ref,
    ig_send, ig_recv, ig_own, rg_ref, ret_ref,
    in_sem, xs_sem, xr_sem, gs_sem, gr_sem, xfs_sem, xfr_sem, gfs_sem, gfr_sem,
    wo_ssem, wo_rsem, ag_ssem, ag_rsem, rs_ssem, rs_rsem, fin_sem, ig_sem, ret_ssem, ret_rsem,
):
    e = lax.axis_index("expert")
    w = lax.axis_index("wide")
    ey, ex = e // SIDE, lax.rem(e, SIDE)
    z, c = w // 2, lax.rem(w, 2)
    other = 1 - c
    partner = (e, z * 2 + other)

    def zdev(step, core):
        return (e, lax.rem(z + step + RING, RING) * 2 + core)

    def edev(dy, dx):
        return lax.rem(ey + dy + SIDE, SIDE) * SIDE + lax.rem(ex + dx + SIDE, SIDE)

    def remote(src, dst, ssem, rsem, dev):
        return pltpu.make_async_remote_copy(
            src_ref=src, dst_ref=dst, send_sem=ssem, recv_sem=rsem,
            device_id=dev, device_id_type=MESH,
        )

    def feat(blk):
        return pl.ds(pl.multiple_of(blk * BLK, BLK), BLK)

    def erow(core, ei):
        return pl.ds(pl.multiple_of(core * ROWS + ei * CAP, CAP), CAP)

    barrier = pltpu.get_barrier_semaphore()
    peers = [(edev(dy, dx), w) for dy, dx in OFFSETS] + [partner]
    peers += [zdev(s, core) for s in (1, -1) for core in (c, other)]
    for dev in peers:
        pl.semaphore_signal(barrier, inc=1, device_id=dev, device_id_type=MESH)

    mine = pl.ds(pl.multiple_of(c * HALF, BLK), HALF)
    theirs = pl.ds(pl.multiple_of(other * HALF, BLK), HALF)
    places = [
        (rt_hbm, rt_ref), (gp_hbm, gp_ref), (tok_hbm, tok_ref),
        (wg_hbm.at[:, mine], wgu_ref.at[feat(w), pl.ds(0, HALF)]),
        (wu_hbm.at[:, mine], wgu_ref.at[feat(w), pl.ds(HALF, HALF)]),
        (wg_hbm.at[:, theirs], wgu_other.at[:, pl.ds(0, HALF)]),
        (wu_hbm.at[:, theirs], wgu_other.at[:, pl.ds(HALF, HALF)]),
        (wd_hbm.at[:, mine], wd_ref.at[feat(w)]),
        (wd_hbm.at[:, theirs], wd_other),
        (og_hbm, og_ref),
    ]
    loads = [pltpu.make_async_copy(a, b, in_sem.at[i]) for i, (a, b) in enumerate(places)]
    for load in loads:
        load.start()

    loads[0].wait()
    loads[1].wait()
    lane = lax.broadcasted_iota(jnp.int32, (EXPERTS, TOK), 0)
    hot = [rt_ref[k:k + 1, :] == lane for k in range(2)]
    named = jnp.where(jnp.logical_or(hot[0], hot[1]), 1.0, 0.0).astype(BF16)
    earlier = jnp.where(
        lax.broadcasted_iota(jnp.int32, (TOK, TOK), 0)
        < lax.broadcasted_iota(jnp.int32, (TOK, TOK), 1), 1.0, 0.0,
    ).astype(BF16)
    before = contract(named, earlier, 1, 0)
    slots = lax.broadcasted_iota(jnp.int32, (ROWS, TOK), 0).astype(F32)
    pick, slot_gate = 0.0, 0.0
    for k in range(2):
        slot = jnp.sum(jnp.where(hot[k], before, 0.0), axis=0, keepdims=True)
        pos = rt_ref[k:k + 1, :].astype(F32) * float(CAP) + slot
        chosen = pos == slots
        pick = pick + jnp.where(chosen, 1.0, 0.0)
        slot_gate = slot_gate + jnp.where(chosen, gp_ref[k:k + 1, :], 0.0)
    slot_gate = jnp.sum(slot_gate, axis=1, keepdims=True)
    pick_ref[...] = pick.astype(BF16)
    loads[2].wait()

    def pick_x(j, carry):
        cols = pl.ds(pl.multiple_of(j * 512, 512), 512)
        send_x[:, cols] = contract(pick_ref[...], tok_ref[:, cols], 1, 0).astype(BF16)
        return carry

    lax.fori_loop(0, 4, pick_x, 0)
    for load in loads[3:9]:
        load.wait()
    pl.semaphore_wait(barrier, len(peers))

    swaps = [
        remote(wgu_other, wgu_ref.at[feat(w)], wo_ssem.at[0], wo_rsem.at[0], partner),
        remote(wd_other, wd_ref.at[feat(w)], wo_ssem.at[1], wo_rsem.at[1], partner),
    ]
    for swap in swaps:
        swap.start()

    def ag_copy(kind, direction, k):
        d = 0 if direction > 0 else 1
        parity = c if (k % 2 == 0) else other
        if k == 6 and direction < 0:
            parity = other
        blk = lax.rem(z - direction * (k // 2) + 2 * RING, RING) * 2 + parity
        ref = (wgu_ref, wd_ref)[kind].at[feat(blk)]
        i = kind * 7 + k
        return remote(ref, ref, ag_ssem.at[d, i], ag_rsem.at[d, i], zdev(direction, c))

    for kind in range(2):
        for direction in (1, -1):
            ag_copy(kind, direction, 0).start()

    own_rows = pl.ds(pl.multiple_of(e * CAP, CAP), CAP)

    def row_copies(src, dst, ssem, rsem):
        out = []
        for i, (dy, dx) in enumerate(OFFSETS):
            dest = edev(dy, dx)
            out.append(remote(
                src.at[pl.ds(pl.multiple_of(dest * CAP, CAP), CAP)],
                dst.at[erow(c, e)], ssem.at[i], rsem.at[i], (dest, w),
            ))
        return out

    x_sends = row_copies(send_x, x_ref, xs_sem, xr_sem)
    for copy in x_sends:
        copy.start()
    x_ref[erow(c, e), :] = send_x[own_rows, :]

    loads[9].wait()

    def pick_g(j, carry):
        cols = pl.ds(pl.multiple_of(j * 512, 512), 512)
        got = contract(pick_ref[...], og_ref[:, cols], 1, 0)
        send_g[:, cols] = (got * slot_gate).astype(BF16)
        return carry

    lax.fori_loop(0, 4, pick_g, 0)
    g_sends = row_copies(send_g, g_ref, gs_sem, gr_sem)
    for copy in g_sends:
        copy.start()
    g_ref[erow(c, e), :] = send_g[own_rows, :]
    for kind in range(2):
        swaps[kind].wait()
        for direction in (1, -1):
            ag_copy(kind, direction, 1).start()

    def forward(buf, ssem, rsem, i, src):
        return remote(buf.at[erow(c, src)], buf.at[erow(c, src)], ssem.at[i], rsem.at[i], partner)

    def pass_on(buf, sends, ssem, rsem, lo, hi):
        for i in range(lo, hi):
            dy, dx = OFFSETS[i]
            sends[i].wait_recv()
            forward(buf, ssem, rsem, i, edev(-dy, -dx)).start()

    def pass_x(lo, hi):
        pass_on(x_ref, x_sends, xfs_sem, xfr_sem, lo, hi)

    def pass_g(lo, hi):
        pass_on(g_ref, g_sends, gfs_sem, gfr_sem, lo, hi)

    def arrived(buf, ssem, rsem):
        for i, (dy, dx) in enumerate(OFFSETS + [(0, 0)]):
            forward(buf, ssem, rsem, i, edev(-dy, -dx)).wait_recv()

    def ag_arrive(kind, k):
        for direction in (1, -1):
            ag_copy(kind, direction, k).wait_recv()
            if direction < 0 and k == 5:
                ag_copy(kind, direction, 6).start()
            elif k + 2 <= 6 and not (direction < 0 and k == 4):
                ag_copy(kind, direction, k + 2).start()

    def add_block(blk, start):
        feats = pl.ds(pl.multiple_of(lax.rem(blk, RING) * 256, 256), 256)

        def tile(t, carry):
            rows = pl.ds(pl.multiple_of(t * 256, 256), 256)
            got = contract(x_ref[rows, feats], wgu_ref[feats, :], 1, 0)
            pre_ref[rows, :] = got if start else pre_ref[rows, :] + got
            return carry

        lax.fori_loop(0, 4, tile, 0)

    def add_more(t, carry):
        add_block(z + RING - 3 + t, False)
        return carry

    def hidden(t, carry):
        rows = pl.ds(pl.multiple_of(t * 32, 32), 32)
        gate_pre = pre_ref[rows, :HALF]
        active = gate_pre * jax.nn.sigmoid(gate_pre)
        hid_ref[rows, :] = (active * pre_ref[rows, HALF:]).astype(BF16)
        return carry

    for k in range(5):
        ag_arrive(0, k)
        ag_arrive(1, k)
        if k == 0:
            forward(x_ref, xfs_sem, xfr_sem, 15, e).start()
            forward(g_ref, gfs_sem, gfr_sem, 15, e).start()
        if k == 3:
            pass_x(0, 8)
        if k == 4:
            pass_x(8, 15)
    ag_arrive(0, 5)
    arrived(x_ref, xfs_sem, xfr_sem)
    add_block(z, True)
    lax.fori_loop(0, 3, add_more, 0)
    ag_arrive(1, 5)
    lax.fori_loop(4, 7, add_more, 0)
    pass_g(0, 6)
    ag_arrive(0, 6)
    add_block(z + 4, False)
    lax.fori_loop(0, 2 * ROWS // 32, hidden, 0)
    ag_arrive(1, 6)
    pass_g(6, 15)

    bufs = ((sd_send, sd_recv), (su_send, su_recv))

    def partial(kind, blk):
        cols = feat(blk)
        if kind == 0:
            return contract(g_ref[:, cols], hid_ref[...], 0, 0)
        return contract(x_ref[:, cols], act_ref[...], 0, 0)

    def rs_parity(direction, k):
        even = lax.rem(k, 2) == 0
        return jnp.where(even, c, other) if direction > 0 else jnp.where(even, other, c)

    def rs_copy(kind, direction, k):
        d = 0 if direction > 0 else 1
        send, recv = bufs[kind]
        core = jnp.where(k >= 5, rs_parity(direction, k), c)
        return remote(
            send.at[d, k], recv.at[d, k], rs_ssem.at[d, kind * 7 + k],
            rs_rsem.at[d, kind * 7 + k], zdev(direction, core),
        )

    def rs_step(kind, k, add):
        send, recv = bufs[kind]
        for direction in (1, -1):
            d = 0 if direction > 0 else 1
            dist = 4 - (k + 1) // 2
            blk = lax.rem(z + direction * dist + RING, RING) * 2 + rs_parity(direction, k)
            got = partial(kind, blk)
            if add:
                rs_copy(kind, direction, k - 2).wait_recv()
                got = got + recv[d, k - 2].astype(F32)
            send[d, k] = got.astype(BF16)
            rs_copy(kind, direction, k).start()

    def rs_loop(kind, lo, hi, add):
        def step(k, carry):
            rs_step(kind, k, add)
            return carry

        lax.fori_loop(lo, hi, step, 0)

    def first_part(direction, core):
        rows = pl.ds(pl.multiple_of(core * ROWS, ROWS), ROWS)
        blk = lax.rem(z + 4, RING) * 2 + (c if direction > 0 else other)
        return contract(g_ref[rows, feat(blk)], hid_ref[rows, :], 0, 0)

    for d, direction in enumerate((1, -1)):
        own_ref[:, d * HALF:(d + 1) * HALF] = first_part(direction, c)
    arrived(g_ref, gfs_sem, gfr_sem)
    for d, direction in enumerate((1, -1)):
        got = own_ref[:, d * HALF:(d + 1) * HALF] + first_part(direction, other)
        sd_send[d, 0] = got.astype(BF16)
        rs_copy(0, direction, 0).start()
    rs_loop(0, 1, 2, False)

    def second(t, carry):
        rows = pl.ds(pl.multiple_of(t * 512, 512), 512)
        hg_ref[rows, :] = contract(g_ref[rows, :], wd_ref[...], 1, 0)
        return carry

    lax.fori_loop(0, 2, second, 0)

    def swish(t, carry):
        rows = pl.ds(pl.multiple_of(t * 32, 32), 32)
        gate_pre = pre_ref[rows, :HALF]
        up_pre = pre_ref[rows, HALF:]
        hidden_grad = hg_ref[rows, :]
        squash = jax.nn.sigmoid(gate_pre)
        act_ref[rows, :HALF] = (
            hidden_grad * up_pre * squash * (1.0 + gate_pre * (1.0 - squash))
        ).astype(BF16)
        act_ref[rows, HALF:] = (hidden_grad * (gate_pre * squash)).astype(BF16)
        return carry

    lax.fori_loop(0, 2 * ROWS // 32, swish, 0)
    rs_loop(1, 0, 2, False)

    def input_part(core, j):
        rows = pl.ds(pl.multiple_of(core * ROWS, ROWS), ROWS)
        cols = pl.ds(pl.multiple_of(j * 256, 256), 256)
        return contract(act_ref[rows, :], wgu_ref[cols, :], 1, 1), cols

    def for_other(j, carry):
        got, cols = input_part(other, j)
        ig_send[:, cols] = got.astype(BF16)
        return carry

    lax.fori_loop(0, 8, for_other, 0)
    ig_copy = remote(ig_send, ig_recv, ig_sem.at[0], ig_sem.at[1], partner)
    ig_copy.start()
    rs_loop(0, 2, 4, True)

    def for_mine(j, carry):
        got, cols = input_part(c, j)
        ig_own[:, cols] = got
        return carry

    lax.fori_loop(0, 8, for_mine, 0)
    ig_copy.wait_recv()

    def join(t, carry):
        rows = pl.ds(pl.multiple_of(t * CAP, CAP), CAP)
        rg_ref[rows, :] = (ig_own[rows, :] + ig_recv[rows, :].astype(F32)).astype(BF16)
        return carry

    lax.fori_loop(0, EXPERTS, join, 0)
    returns = []
    for i, (dy, dx) in enumerate(OFFSETS):
        dest = edev(dy, dx)
        returns.append(remote(
            rg_ref.at[pl.ds(pl.multiple_of(dest * CAP, CAP), CAP)],
            ret_ref.at[own_rows], ret_ssem.at[i], ret_rsem.at[i], (dest, w),
        ))
    for copy in returns:
        copy.start()
    ret_ref[own_rows, :] = rg_ref[own_rows, :]

    def rs_rest(k, carry):
        rs_step(1, k, True)

        @pl.when(k <= 4)
        def _():
            rs_step(0, k + 2, True)

        return carry

    lax.fori_loop(2, 4, rs_rest, 0)

    fin_send[:, :F] = partial(1, z * 2 + other).astype(BF16)
    fin_send[:, F:] = partial(0, z * 2 + other).astype(BF16)
    fin = remote(fin_send, fin_recv, fin_sem.at[0], fin_sem.at[1], partner)
    fin.start()
    lax.fori_loop(4, 7, rs_rest, 0)
    own_ref[:, :F] = partial(1, w)
    own_ref[:, F:] = partial(0, w)

    for copy in returns:
        copy.wait_recv()

    def combine(j, carry):
        cols = pl.ds(pl.multiple_of(j * 512, 512), 512)
        gi_ref[:, cols] = contract(pick_ref[...], ret_ref[:, cols], 0, 0).astype(BF16)
        return carry

    lax.fori_loop(0, 4, combine, 0)
    fin.wait_recv()

    for kind in range(2):
        recv = bufs[kind][1]
        for direction in (1, -1):
            for k in (5, 6):
                rs_copy(kind, direction, k).wait_recv()
        outs = ((gd_ref, F),) if kind == 0 else ((gg_ref, 0), (gu_ref, HALF))
        for i, (out, lo) in enumerate(outs):
            part = slice(i * HALF, (i + 1) * HALF)
            out[:, mine] = (
                own_ref[:, lo:lo + HALF]
                + recv[0, 6, :, part].astype(F32) + recv[1, 5, :, part].astype(F32)
            )
            out[:, theirs] = (
                fin_recv[:, lo:lo + HALF].astype(F32)
                + recv[0, 5, :, part].astype(F32) + recv[1, 6, :, part].astype(F32)
            )

    for copy in x_sends + g_sends + returns:
        copy.wait_send()
    for i, (dy, dx) in enumerate(OFFSETS + [(0, 0)]):
        src = edev(-dy, -dx)
        forward(x_ref, xfs_sem, xfr_sem, i, src).wait_send()
        forward(g_ref, gfs_sem, gfr_sem, i, src).wait_send()
    for direction in (1, -1):
        for k in range(7):
            for kind in range(2):
                ag_copy(kind, direction, k).wait_send()
                rs_copy(kind, direction, k).wait_send()
    ig_copy.wait_send()
    fin.wait_send()


def store(*refs):
    n = len(refs) // 2
    sem = refs[-1]
    copies = [pltpu.make_async_copy(refs[i], refs[n + i], sem.at[i]) for i in range(n)]
    for copy in copies:
        copy.start()
    for copy in copies:
        copy.wait()


def on_device(tokens, out_grad, routes, gate_prob, w_gate, w_up, w_down):
    flat = [a.reshape(BLK, F) for a in (w_gate, w_up, w_down)]
    dma = pltpu.SemaphoreType.DMA
    vmem = pl.BlockSpec(memory_space=pltpu.VMEM)
    anyw = pl.BlockSpec(memory_space=pl.ANY)
    shapes = [((TOK, D), BF16)] + [((BLK, F), F32)] * 3
    outs = pl.pallas_call(
        kernel,
        name="moe_back",
        out_shape=tuple(pltpu.VMEM(s, t) for s, t in shapes),
        in_specs=[anyw] * 7,
        out_specs=(vmem,) * 4,
        scratch_shapes=[
            pltpu.VMEM((TOK, D), BF16),
            pltpu.VMEM((TOK, D), BF16),
            pltpu.VMEM((2, TOK), jnp.int32),
            pltpu.VMEM((2, TOK), F32),
            pltpu.VMEM((ROWS, D), BF16),
            pltpu.VMEM((ROWS, D), BF16),
            pltpu.VMEM((2 * ROWS, D), BF16),
            pltpu.VMEM((2 * ROWS, D), BF16),
            pltpu.VMEM((D, F), BF16),
            pltpu.VMEM((D, HALF), BF16),
            pltpu.VMEM((BLK, F), BF16),
            pltpu.VMEM((BLK, HALF), BF16),
            pltpu.VMEM((ROWS, TOK), BF16),
            pltpu.VMEM((2 * ROWS, F), F32),
            pltpu.VMEM((2 * ROWS, HALF), F32),
            pltpu.VMEM((2 * ROWS, F), BF16),
            pltpu.VMEM((2 * ROWS, HALF), BF16),
            pltpu.VMEM((2, 7, BLK, HALF), BF16),
            pltpu.VMEM((2, 7, BLK, HALF), BF16),
            pltpu.VMEM((2, 7, BLK, F), BF16),
            pltpu.VMEM((2, 7, BLK, F), BF16),
            pltpu.VMEM((BLK, TRIP), BF16),
            pltpu.VMEM((BLK, TRIP), BF16),
            pltpu.VMEM((BLK, TRIP), F32),
            pltpu.VMEM((ROWS, D), BF16),
            pltpu.VMEM((ROWS, D), BF16),
            pltpu.VMEM((ROWS, D), F32),
            pltpu.VMEM((ROWS, D), BF16),
            pltpu.VMEM((ROWS, D), BF16),
            dma((10,)),
            dma((15,)), dma((15,)), dma((15,)), dma((15,)),
            dma((16,)), dma((16,)), dma((16,)), dma((16,)),
            dma((2,)), dma((2,)), dma((2, 14)), dma((2, 14)), dma((2, 14)), dma((2, 14)),
            dma((2,)), dma((2,)), dma((15,)), dma((15,)),
        ],
        compiler_params=pltpu.CompilerParams(
            collective_id=0, has_side_effects=True, vmem_limit_bytes=56 << 20,
        ),
    )(tokens, out_grad, routes.T, gate_prob.T, *flat)
    outs = pl.pallas_call(
        store,
        name="store",
        out_shape=tuple(jax.ShapeDtypeStruct(s, t) for s, t in shapes),
        in_specs=[vmem] * 4,
        out_specs=(anyw,) * 4,
        scratch_shapes=[dma((4,))],
        compiler_params=pltpu.CompilerParams(vmem_limit_bytes=4 << 20),
    )(*outs)
    return (outs[0],) + tuple(o[None] for o in outs[1:])


def solution(mesh):
    rows = P(("expert", "wide"), None)
    weight = P("expert", "wide", None)
    return jax.shard_map(
        on_device,
        mesh=mesh,
        in_specs=(rows,) * 4 + (weight,) * 3,
        out_specs=(rows,) + (weight,) * 3,
        check_vma=False,
    )
```
